32 devices in a mesh: ctx: 8 (over z, x), head: 4 (over y, core).
Axes of the slice: x: 2, y: 2, z: 4, core: 2. Of those that a mesh axis runs over, the one named last changes fastest.
Arguments:
- query: bfloat16 [6144, 1024], P('ctx', 'head'), parts along dimension 1, may hold values from -6 to 6
- key_value: bfloat16 [6144, 1024], P('ctx', 'head'), parts along dimension 1, may hold values from -6 to 6
- d_out: bfloat16 [6144, 1024], P('ctx', 'head'), parts along dimension 1, may hold values from -128 to 128
- doc_starts: int32 [64], P('head'), parts along dimension 0, may hold values from 0 to 6143, as said below
Outputs:
- d_query: bfloat16 [6144, 1024], P('ctx', 'head'), parts along dimension 1
- d_key_value: bfloat16 [6144, 1024], P('ctx', 'head'), parts along dimension 1
The draws below stay inside these ranges and needn't reach their ends.
There are 4 independent parts, one for each index of `head`. The reference program is written for one: setup_inputs(seed, part) draws one part's arguments, and reference() takes and returns one part's arrays. A program takes and returns all parts, laid end to end along the dimension named above; each array names one. Nothing has to cross between parts.
Inputs may be any that keep to these rules, and one draw needn't show every extreme that they name: `doc_starts`: Non-decreasing, first entry 0; the document of position p runs from the largest entry not above p up to the next larger entry or 6144; repeated entries are empty documents. A position p never belongs to a document that begins before (p // 768 - 3) * 768, and in every draw some document begins in the block of 768 positions exactly 3 blocks before the block of its last position.
All inputs are finite; a program needn't handle non-finite values.
Results may differ from the reference program's by a relative error of at most 0.0055.
Values may be sent and summed in bfloat16 or wider, within the bound.
A program may use at most 128 MiB of HBM per device.

```python
import jax
import jax.numpy as jnp
from jax import lax

HD = 128
QH = 2
HOPS = 3
TOK_DEV = 768
TOKENS = 6144
STARTS = 16


def start_list(key):
    base = jax.random.fold_in(key, 7001)
    key_offsets, key_anchor, key_coin, key_long = jax.random.split(base, 4)
    half_block = TOK_DEV // 2
    count = STARTS
    group_size = HOPS
    group_count = (count + group_size - 1) // group_size
    strata = jnp.arange(count, dtype=jnp.int32)
    offsets = jax.random.randint(key_offsets, (count,), 0, half_block, dtype=jnp.int32)
    anchor_pick = jax.random.randint(key_anchor, (group_count,), 0, group_size, dtype=jnp.int32)
    anchors = jnp.minimum(jnp.arange(group_count, dtype=jnp.int32) * group_size + anchor_pick, count - 1)
    is_anchor = anchors[strata // group_size] == strata
    coins = jax.random.randint(key_coin, (count,), 0, 2, dtype=jnp.int32) == 1
    keeping = is_anchor | coins | (strata == 0)
    options = (count // group_size - 1) // 2
    long_group = 2 * jax.random.randint(key_long, (), 0, options, dtype=jnp.int32) + 1
    lower = long_group * group_size
    upper = (long_group + 2) * group_size - 1
    inside = (strata > lower) & (strata < upper)
    keeping = jnp.where(inside, False, keeping) | (strata == lower) | (strata == upper)
    offsets = jnp.where(strata == lower, 0, jnp.where(strata == upper, half_block - 1, offsets))
    offsets = jnp.where(strata == 0, 0, offsets)
    cuts = strata * half_block + offsets
    return lax.cummax(jnp.where(keeping, cuts, 0), axis=0).astype(jnp.int32)


def query_and_pairs(key):
    base = jax.random.fold_in(key, 7002)
    key_query, key_keys, key_values = jax.random.split(base, 3)
    queries = jnp.clip(jax.random.normal(key_query, (TOKENS, QH * HD), jnp.float32), -6.0, 6.0)
    keys_drawn = jnp.clip(jax.random.normal(key_keys, (TOKENS, HD), jnp.float32), -6.0, 6.0)
    values_drawn = jnp.clip(jax.random.normal(key_values, (TOKENS, HD), jnp.float32), -6.0, 6.0)
    return (queries, jnp.concatenate([keys_drawn, values_drawn], axis=1))


def draw_query(key, part):
    return query_and_pairs(key)[0].astype(jnp.bfloat16)


def draw_key_value(key, part):
    return query_and_pairs(key)[1].astype(jnp.bfloat16)


def draw_doc_starts(key, part):
    return start_list(key)


def shard_levels(rng, dims, cuts, low, top_value):
    def one(dim, blocks):
        steps = jax.random.uniform(jax.random.fold_in(jax.random.fold_in(rng, 6), dim), (blocks,), jnp.float32, low / len(cuts), top_value / len(cuts))
        return jnp.repeat(jnp.exp(steps), dims[dim] // blocks).reshape((-1,) + (1,) * (len(dims) - dim - 1))

    factor_of = one(*cuts[0])
    for cut in cuts[1:]:
        factor_of = factor_of * one(*cut)
    return factor_of


def normal_values(stream_key, dims, spread, bound, cuts=(), kind=jnp.bfloat16):
    values = spread * jax.random.normal(stream_key, dims, jnp.float32)
    if cuts:
        values = values * shard_levels(stream_key, dims, cuts, -0.22, 0.18)
    return jnp.clip(values, -bound, bound).astype(kind)


def setup_inputs(seed: int = 0, part: int = 0) -> dict:
    key_of = jax.random.split(jax.random.key(seed), 5)
    part_splits = jax.random.split(jax.random.fold_in(key_of[4], part), 5)
    return {
        "query": draw_query(jax.random.fold_in(jax.random.fold_in(key_of[4], part), 71), part),
        "key_value": draw_key_value(jax.random.fold_in(jax.random.fold_in(key_of[4], part), 71), part),
        "d_out": normal_values(part_splits[2], (TOKENS, QH * HD), 24.0, 128.0, ((0, 8),)),
        "doc_starts": draw_doc_starts(jax.random.fold_in(jax.random.fold_in(key_of[4], part), 71), part),
    }


def start_of(doc_starts, positions):
    earlier = doc_starts[None, :] <= positions[:, None]
    return jnp.max(jnp.where(earlier, doc_starts[None, :], 0), axis=1).astype(jnp.int32)


def reference(query, key_value, d_out, doc_starts):
    score_scale = HD ** -0.5
    reach = HOPS * TOK_DEV
    window = reach + TOK_DEV
    padded = jnp.concatenate([jnp.zeros((reach, 2 * HD), key_value.dtype), key_value], axis=0)

    def block_terms(block_index):
        first_row = (block_index * TOK_DEV).astype(jnp.int32)
        queries = lax.dynamic_slice_in_dim(query, first_row, TOK_DEV, 0).reshape(TOK_DEV, QH, HD).astype(jnp.float32)
        grads_out = lax.dynamic_slice_in_dim(d_out, first_row, TOK_DEV, 0).reshape(TOK_DEV, QH, HD).astype(jnp.float32)
        kv_window = lax.dynamic_slice_in_dim(padded, first_row, window, 0)
        key_block = kv_window[:, :HD].astype(jnp.float32)
        value_block = kv_window[:, HD:].astype(jnp.float32)
        query_pos = first_row + jnp.arange(TOK_DEV, dtype=jnp.int32)
        key_pos = first_row - reach + jnp.arange(window, dtype=jnp.int32)
        owners = start_of(doc_starts, query_pos)
        visible = ((key_pos[None, :] >= owners[:, None]) & (key_pos[None, :] <= query_pos[:, None]))[None]
        scores = jnp.einsum("thd,sd->hts", queries, key_block) * score_scale
        row_top = jnp.max(jnp.where(visible, scores, -jnp.inf), axis=2)
        row_total = jnp.sum(jnp.where(visible, jnp.exp(scores - row_top[:, :, None]), 0.0), axis=2)
        log_total = row_top + jnp.log(row_total)
        weights = jnp.where(visible, jnp.exp(scores - log_total[:, :, None]), 0.0)
        grad_prob = jnp.einsum("thd,sd->hts", grads_out, value_block)
        row_delta = jnp.sum(weights * grad_prob, axis=2)
        grad_score = (weights * (grad_prob - row_delta[:, :, None]) * score_scale).astype(jnp.bfloat16)
        grad_score = lax.optimization_barrier(grad_score).astype(jnp.float32)
        low_weights = lax.optimization_barrier(weights.astype(jnp.bfloat16)).astype(jnp.float32)
        grad_query = jnp.einsum("hts,sd->thd", grad_score, key_block).reshape(TOK_DEV, QH * HD).astype(jnp.bfloat16)
        grad_key = jnp.einsum("hts,thd->sd", grad_score, queries)
        grad_value = jnp.einsum("hts,thd->sd", low_weights, grads_out)
        shares = jnp.concatenate([grad_key, grad_value], axis=1).astype(jnp.bfloat16)
        shares = lax.optimization_barrier(shares).astype(jnp.float32)
        return grad_query, shares

    def advance(carried, block_index):
        grad_query, shares = block_terms(block_index)
        first_row = (block_index * TOK_DEV).astype(jnp.int32)
        current = lax.dynamic_slice_in_dim(carried, first_row, window, 0)
        carried = lax.dynamic_update_slice_in_dim(carried, current + shares, first_row, 0)
        return carried, grad_query

    blocks = TOKENS // TOK_DEV
    initial = jnp.zeros((reach + TOKENS, 2 * HD), jnp.float32)
    carried, grad_queries = lax.scan(advance, initial, jnp.arange(blocks, dtype=jnp.int32))
    return grad_queries.reshape(TOKENS, QH * HD), carried[reach:].astype(jnp.bfloat16)
```

```python
import functools
import math

import jax
import jax.numpy as jnp
from jax import lax
from jax.experimental import pallas as pl
from jax.experimental.pallas import tpu as pltpu
from jax.sharding import PartitionSpec as P

HOPS = 3
NEG = -1e30
SUB = 2
KEY_TILES = 4
MESH = pl.DeviceIdType.MESH


def dot_nt(a, b):
    return lax.dot_general(a, b, (((1,), (1,)), ((), ())), preferred_element_type=jnp.float32)


def dot(a, b):
    return jnp.dot(a, b, preferred_element_type=jnp.float32)


def kernel(
    n, q_ref, g_ref, kv_ref, ds_ref, dq_ref, dkv_ref,
    got, expo, gprob, top, total, weighted, factor, delta, low_p, low_g, dq_t, own, share, back,
    own_rows, f_send, f_recv, b_send, b_recv,
):
    me = lax.axis_index("ctx")
    odd = lax.rem(me, 2)
    is_odd, is_even = odd == 1, odd == 0
    tok, width = q_ref.shape
    hd = kv_ref.shape[1] // 2
    heads = width // hd
    half = tok // 2
    piece = half // SUB
    kt_rows = tok // KEY_TILES
    qt = math.gcd(tok, 256)
    scale = hd ** -0.5
    to_log2 = scale * math.log2(math.e)
    has_next = me + 2 < n

    barrier = pltpu.get_barrier_semaphore()
    pair = me + 1 - 2 * odd

    def greet(device):
        pl.semaphore_signal(barrier, inc=1, device_id={"ctx": device}, device_id_type=MESH)

    greet(pair)

    @pl.when(has_next)
    def _():
        greet(me + 2)

    @pl.when(me >= 2)
    def _():
        greet(me - 2)

    @pl.when(has_next & (me >= 2))
    def _():
        pl.semaphore_wait(barrier, 3)

    @pl.when(jnp.logical_not(has_next & (me >= 2)))
    def _():
        pl.semaphore_wait(barrier, 2)

    def rows_of(c):
        return pl.ds(c * piece, piece)

    FIRST, SECOND = range(SUB), range(SUB, 2 * SUB)
    ALL = range(2 * SUB)

    def fwd(slot, src, device, t, c):
        return pltpu.make_async_remote_copy(
            src_ref=src.at[rows_of(c)], dst_ref=got.at[t - 1, rows_of(c)],
            send_sem=f_send.at[slot, c], recv_sem=f_recv.at[t - 1, c],
            device_id={"ctx": device}, device_id_type=MESH,
        )

    def arrived(t, c):
        fwd(0, kv_ref, pair, t, c).wait_recv()

    def when(cond, f):
        pl.when(cond)(f)

    @pl.when(is_even)
    def _():
        for c in list(SECOND) + list(FIRST):
            fwd(0, kv_ref, me + 1, 1, c).start()

        @pl.when(has_next)
        def _():
            for c in FIRST:
                fwd(1, kv_ref, me + 2, 2, c).start()

    @pl.when(is_odd & has_next)
    def _():
        for c in ALL:
            fwd(1, kv_ref, me + 2, 2, c).start()

    position = me * tok + lax.broadcasted_iota(jnp.int32, (1, tok), 1)
    owners = jnp.zeros((1, tok), jnp.int32)
    for i in range(ds_ref.shape[0]):
        start = ds_ref[i]
        owners = jnp.maximum(owners, jnp.where(position >= start, start, 0))
    own_rows[...] = owners
    top[...] = jnp.full(top.shape, NEG, jnp.float32)
    total[...] = jnp.zeros_like(total)
    weighted[...] = jnp.zeros_like(weighted)
    dq_t[...] = jnp.zeros_like(dq_t)

    def tiles():
        for h in range(heads):
            for j in range(tok // qt):
                yield h, j, slice(j * qt, (j + 1) * qt), slice(h * hd, (h + 1) * hd), slice(
                    h * tok + j * qt, h * tok + (j + 1) * qt)

    def block(t):
        return kv_ref if t == 0 else got.at[t - 1]

    def absorb(t, kt):
        r0 = kt * kt_rows
        rows = slice(r0, r0 + kt_rows)
        src = block(t)
        k, v = src[rows, :hd], src[rows, hd:]
        base = (me - t) * tok + r0
        stat = t * KEY_TILES + kt
        key_row = lax.broadcasted_iota(jnp.int32, (kt_rows, qt), 0)
        for h, j, qrows, cols, flat in tiles():
            if t == 0 and (j + 1) * qt <= r0:
                continue
            s = dot_nt(k, q_ref[qrows, cols]) * to_log2
            gp = dot_nt(v, g_ref[qrows, cols]) * scale
            visible = key_row >= own_rows[:, qrows] - base
            if t == 0:
                query_row = lax.broadcasted_iota(jnp.int32, (1, qt), 1) + (j * qt - r0)
                visible = visible & (key_row <= query_row)
            s = jnp.where(visible, s, NEG)
            m = jnp.max(s, axis=0, keepdims=True)
            e = jnp.exp2(s - m)
            expo[t, rows, flat] = e
            gprob[t, rows, flat] = gp
            top[stat : stat + 1, flat] = m
            total[stat : stat + 1, flat] = jnp.sum(e, axis=0, keepdims=True)
            weighted[stat : stat + 1, flat] = jnp.sum(e * gp, axis=0, keepdims=True)

    per_half = KEY_TILES // 2

    def absorb_half(t, which):
        def run():
            for kt in range(which * per_half, (which + 1) * per_half):
                absorb(t, kt)

        if t == 0:
            run()
        else:
            when(me >= t, run)

    absorb_half(0, 0)
    absorb_half(0, 1)

    @pl.when(is_even & (me >= 2))
    def _():
        for c in FIRST:
            arrived(2, c)
            fwd(3, got.at[1], me + 1, 3, c).start()

    @pl.when(is_odd)
    def _():
        for i in range(SUB):
            arrived(1, SECOND[i])

            @pl.when(has_next)
            def _():
                fwd(2, got.at[0], me + 2, 3, SECOND[i]).start()

            @pl.when(me >= 2)
            def _():
                arrived(2, FIRST[i])
                fwd(3, got.at[1], me - 1, 1, FIRST[i]).start()

    absorb_half(2, 0)

    @pl.when(is_odd)
    def _():
        @pl.when(me >= 2)
        def _():
            for c in SECOND:
                arrived(2, c)
                fwd(3, got.at[1], me - 1, 1, c).start()

        for c in FIRST:
            arrived(1, c)

    def relay_first(chunks):
        @pl.when(is_even & (me >= 2))
        def _():
            for c in chunks:
                arrived(1, c)

                @pl.when(has_next)
                def _():
                    fwd(2, got.at[0], me + 2, 3, c).start()

    relay_first(FIRST)
    absorb_half(1, 0)
    relay_first(SECOND)
    absorb_half(1, 1)

    @pl.when(is_odd & (me >= 3))
    def _():
        for c in SECOND:
            arrived(3, c)
            fwd(4, got.at[2], me - 1, 2, c).start()

    @pl.when(me >= 3)
    def _():
        for c in FIRST:
            arrived(3, c)

    @pl.when(is_odd & (me >= 3))
    def _():
        absorb_half(2, 1)

    @pl.when(me >= 3)
    def _():
        absorb_half(3, 0)

    @pl.when(is_even & (me >= 2))
    def _():
        for c in SECOND:
            arrived(2, c)
        absorb_half(2, 1)

    @pl.when(is_even & (me >= 3))
    def _():
        for c in SECOND:
            arrived(3, c)

    absorb_half(3, 1)

    best = jnp.max(top[...], axis=0, keepdims=True)
    grow = jnp.exp2(top[...] - best)
    inverse = 1.0 / jnp.sum(grow * total[...], axis=0, keepdims=True)
    factor[...] = grow * inverse
    delta[...] = jnp.sum(grow * weighted[...], axis=0, keepdims=True) * inverse

    def gradients(t, kt):
        r0 = kt * kt_rows
        rows = slice(r0, r0 + kt_rows)
        slot = kt % 2
        stat = t * KEY_TILES + kt
        first = (r0 // qt) * qt if t == 0 else 0
        for h, j, qrows, cols, flat in tiles():
            if j * qt < first:
                continue
            p = expo[t, rows, flat] * factor[stat : stat + 1, flat]
            low_p[slot, :, flat] = p.astype(jnp.bfloat16)
            low_g[slot, :, flat] = (p * (gprob[t, rows, flat] - delta[:, flat])).astype(jnp.bfloat16)
        dk = dv = None
        k_t = block(t)[rows, :hd].T
        for h in range(heads):
            flat = slice(h * tok + first, (h + 1) * tok)
            cols = slice(h * hd, (h + 1) * hd)
            gs = low_g[slot, :, flat]
            dk_h = dot(gs, q_ref[first:, cols])
            dv_h = dot(low_p[slot, :, flat], g_ref[first:, cols])
            dk = dk_h if dk is None else dk + dk_h
            dv = dv_h if dv is None else dv + dv_h
            dq_t[:, flat] += dot(k_t, gs)
        if t == 0:
            own[rows, :hd] = dk
            own[rows, hd:] = dv
        else:
            share[t - 1, rows, :hd] = dk.astype(jnp.bfloat16)
            share[t - 1, rows, hd:] = dv.astype(jnp.bfloat16)

    def gradients_half(t, which):
        def run():
            for kt in range(which * per_half, (which + 1) * per_half):
                gradients(t, kt)

        if t == 0:
            run()
        else:
            when(me >= t, run)

    def bwd(t, device, slot, c):
        return pltpu.make_async_remote_copy(
            src_ref=share.at[t - 1, rows_of(c)], dst_ref=back.at[slot, rows_of(c)],
            send_sem=b_send.at[t - 1, c], recv_sem=b_recv.at[slot, c],
            device_id={"ctx": device}, device_id_type=MESH,
        )

    def returned(slot, c):
        bwd(1, pair, slot, c).wait_recv()

    def merge(t, c):
        returned(t - 1, c)
        rows = rows_of(c)
        both = share[t - 1, rows, :].astype(jnp.float32) + back[t - 1, rows, :].astype(jnp.float32)
        share[t - 1, rows, :] = both.astype(jnp.bfloat16)

    gradients_half(3, 0)

    @pl.when(me >= 3)
    def _():
        @pl.when(is_even)
        def _():
            for c in FIRST:
                bwd(3, me - 2, 0, c).start()

        @pl.when(is_odd)
        def _():
            for c in FIRST:
                bwd(3, me - 1, 1, c).start()

    gradients_half(2, 1)

    @pl.when(is_even & (me >= 2))
    def _():
        for c in SECOND:
            bwd(2, me + 1, 2, c).start()

    gradients_half(3, 1)

    @pl.when(me >= 3)
    def _():
        @pl.when(is_even)
        def _():
            for c in SECOND:
                bwd(3, me - 2, 0, c).start()

        @pl.when(is_odd)
        def _():
            for c in SECOND:
                merge(3, c)
                bwd(3, me - 2, 0, c).start()

    gradients_half(2, 0)

    @pl.when(is_even & (me >= 2))
    def _():
        for c in FIRST:
            merge(2, c)
            bwd(2, me - 2, 4, c).start()

    def send_one(chunks, add_odd):
        @pl.when(is_even & (me >= 2))
        def _():
            for c in chunks:
                @pl.when(has_next)
                def _():
                    merge(1, c)

                bwd(1, me + 1, 1, c).start()

        @pl.when(is_odd)
        def _():
            for c in chunks:
                if add_odd:
                    @pl.when(has_next)
                    def _():
                        merge(1, c)

                bwd(1, me - 1, 3, c).start()

    gradients_half(1, 0)
    send_one(FIRST, False)
    gradients_half(1, 1)
    send_one(SECOND, True)
    gradients_half(0, 0)
    gradients_half(0, 1)

    @pl.when(is_odd & (me >= 2))
    def _():
        for c in ALL:
            merge(2, c)
            bwd(2, me - 2, 4, c).start()

    for h in range(heads):
        dq_ref[:, h * hd : (h + 1) * hd] = dq_t[:, h * tok : (h + 1) * tok].T.astype(jnp.bfloat16)

    def add_back(slot, c):
        returned(slot, c)
        rows = rows_of(c)
        own[rows, :] += back[slot, rows, :].astype(jnp.float32)

    @pl.when(is_even)
    def _():
        for c in ALL:
            add_back(3, c)

        @pl.when(has_next)
        def _():
            for c in FIRST:
                add_back(4, c)

    @pl.when(is_odd & has_next)
    def _():
        for c in ALL:
            add_back(4, c)

    dkv_ref[...] = own[...].astype(jnp.bfloat16)

    def sent(slot, chunks):
        for c in chunks:
            fwd(slot, kv_ref, pair, 1, c).wait_send()

    def sent_back(t, chunks):
        for c in chunks:
            bwd(t, pair, 0, c).wait_send()

    @pl.when(is_even)
    def _():
        sent(0, ALL)

        @pl.when(has_next)
        def _():
            sent(1, FIRST)

        @pl.when(me >= 2)
        def _():
            sent(3, FIRST)

            @pl.when(has_next)
            def _():
                sent(2, ALL)

    @pl.when(is_odd)
    def _():
        @pl.when(has_next)
        def _():
            sent(1, ALL)
            sent(2, SECOND)

        @pl.when(me >= 2)
        def _():
            sent(3, ALL)
            sent(4, SECOND)

    for t in range(1, HOPS + 1):
        when(me >= t, functools.partial(sent_back, t, ALL))


def shards(n, query, key_value, d_out, doc_starts):
    tok, width = query.shape
    hd = key_value.shape[1] // 2
    flat = tok * (width // hd)
    blocks = HOPS + 1
    stats = blocks * KEY_TILES
    bf16, f32 = jnp.bfloat16, jnp.float32
    vmem = pl.BlockSpec(memory_space=pltpu.VMEM)
    pieces = 2 * SUB
    return pl.pallas_call(
        functools.partial(kernel, n),
        out_shape=(
            jax.ShapeDtypeStruct(query.shape, bf16),
            jax.ShapeDtypeStruct(key_value.shape, bf16),
        ),
        in_specs=[vmem, vmem, vmem, pl.BlockSpec(memory_space=pltpu.SMEM)],
        out_specs=(vmem, vmem),
        scratch_shapes=[
            pltpu.VMEM((HOPS, tok, 2 * hd), bf16),
            pltpu.VMEM((blocks, tok, flat), f32),
            pltpu.VMEM((blocks, tok, flat), f32),
            pltpu.VMEM((stats, flat), f32),
            pltpu.VMEM((stats, flat), f32),
            pltpu.VMEM((stats, flat), f32),
            pltpu.VMEM((stats, flat), f32),
            pltpu.VMEM((1, flat), f32),
            pltpu.VMEM((2, tok // KEY_TILES, flat), bf16),
            pltpu.VMEM((2, tok // KEY_TILES, flat), bf16),
            pltpu.VMEM((hd, flat), f32),
            pltpu.VMEM((tok, 2 * hd), f32),
            pltpu.VMEM((HOPS, tok, 2 * hd), bf16),
            pltpu.VMEM((5, tok, 2 * hd), bf16),
            pltpu.VMEM((1, tok), jnp.int32),
            pltpu.SemaphoreType.DMA((5, pieces)),
            pltpu.SemaphoreType.DMA((HOPS, pieces)),
            pltpu.SemaphoreType.DMA((HOPS, pieces)),
            pltpu.SemaphoreType.DMA((5, pieces)),
        ],
        compiler_params=pltpu.CompilerParams(
            collective_id=0, has_side_effects=True, vmem_limit_bytes=63 * 2**20
        ),
    )(query, d_out, key_value, doc_starts)


def solution(mesh):
    placed = (P("ctx", "head"), P("ctx", "head"), P("ctx", "head"), P("head"))
    return jax.shard_map(
        functools.partial(shards, mesh.shape["ctx"]),
        mesh=mesh,
        in_specs=placed,
        out_specs=(P("ctx", "head"), P("ctx", "head")),
        check_vma=False,
    )
```

```python
import functools
import math

import jax
import jax.numpy as jnp
from jax import lax
from jax.experimental import pallas as pl
from jax.experimental.pallas import tpu as pltpu
from jax.sharding import PartitionSpec as P

HOPS = 3
NEG = -1e30
KEY_TILES = 4
SUB = 2
FIRST, SECOND = range(3), range(3, 4)
MESH = pl.DeviceIdType.MESH


def dot_nt(a, b):
    return lax.dot_general(a, b, (((1,), (1,)), ((), ())), preferred_element_type=jnp.float32)


def dot(a, b):
    return jnp.dot(a, b, preferred_element_type=jnp.float32)


def kernel(
    n, q_ref, g_ref, kv_ref, ds_ref, dq_ref, dkv_ref,
    got, expo, gprob, top, total, weighted, factor, delta, low_p, low_g, dq_t, own, share, back,
    own_rows, f_send, f_recv, b_send, b_recv,
):
    me = lax.axis_index("ctx")
    odd = lax.rem(me, 2)
    is_odd, is_even = odd == 1, odd == 0
    tok, width = q_ref.shape
    hd = kv_ref.shape[1] // 2
    heads = width // hd
    kt_rows = tok // KEY_TILES
    piece = kt_rows // SUB
    qt = math.gcd(tok, 256)
    scale = hd ** -0.5
    to_log2 = scale * math.log2(math.e)
    has_next = me + 2 < n

    barrier = pltpu.get_barrier_semaphore()
    pair = me + 1 - 2 * odd

    def greet(device):
        pl.semaphore_signal(barrier, inc=1, device_id={"ctx": device}, device_id_type=MESH)

    greet(pair)

    @pl.when(has_next)
    def _():
        greet(me + 2)

    @pl.when(me >= 2)
    def _():
        greet(me - 2)

    @pl.when(has_next & (me >= 2))
    def _():
        pl.semaphore_wait(barrier, 3)

    @pl.when(jnp.logical_not(has_next & (me >= 2)))
    def _():
        pl.semaphore_wait(barrier, 2)

    def rows_of(c):
        return pl.ds(c * piece, piece)

    def pieces(kts):
        return [kt * SUB + i for kt in kts for i in range(SUB)]

    ALL = range(KEY_TILES)

    def fwd(slot, src, device, t, c):
        return pltpu.make_async_remote_copy(
            src_ref=src.at[rows_of(c)], dst_ref=got.at[t - 1, rows_of(c)],
            send_sem=f_send.at[slot, c], recv_sem=f_recv.at[t - 1, c],
            device_id={"ctx": device}, device_id_type=MESH,
        )

    def arrived(t, c):
        fwd(0, kv_ref, pair, t, c).wait_recv()

    def when(cond, f):
        pl.when(cond)(f)

    @pl.when(is_even)
    def _():
        for c in pieces(SECOND) + pieces(FIRST):
            fwd(0, kv_ref, me + 1, 1, c).start()

        @pl.when(has_next)
        def _():
            for c in pieces(FIRST):
                fwd(1, kv_ref, me + 2, 2, c).start()

    @pl.when(is_odd & has_next)
    def _():
        for c in pieces(ALL):
            fwd(1, kv_ref, me + 2, 2, c).start()

    position = me * tok + lax.broadcasted_iota(jnp.int32, (1, tok), 1)
    owners = jnp.zeros((1, tok), jnp.int32)
    for i in range(ds_ref.shape[0]):
        start = ds_ref[i]
        owners = jnp.maximum(owners, jnp.where(position >= start, start, 0))
    own_rows[...] = owners
    top[...] = jnp.full(top.shape, NEG, jnp.float32)
    total[...] = jnp.zeros_like(total)
    weighted[...] = jnp.zeros_like(weighted)
    dq_t[...] = jnp.zeros_like(dq_t)

    def tiles():
        for h in range(heads):
            for j in range(tok // qt):
                yield h, j, slice(j * qt, (j + 1) * qt), slice(h * hd, (h + 1) * hd), slice(
                    h * tok + j * qt, h * tok + (j + 1) * qt)

    def block(t):
        return kv_ref if t == 0 else got.at[t - 1]

    def absorb(t, kt):
        r0 = kt * kt_rows
        rows = slice(r0, r0 + kt_rows)
        src = block(t)
        k, v = src[rows, :hd], src[rows, hd:]
        base = (me - t) * tok + r0
        stat = t * KEY_TILES + kt
        key_row = lax.broadcasted_iota(jnp.int32, (kt_rows, qt), 0)
        for h, j, qrows, cols, flat in tiles():
            if t == 0 and (j + 1) * qt <= r0:
                continue
            s = dot_nt(k, q_ref[qrows, cols]) * to_log2
            gp = dot_nt(v, g_ref[qrows, cols]) * scale
            visible = key_row >= own_rows[:, qrows] - base
            if t == 0:
                query_row = lax.broadcasted_iota(jnp.int32, (1, qt), 1) + (j * qt - r0)
                visible = visible & (key_row <= query_row)
            s = jnp.where(visible, s, NEG)
            m = jnp.max(s, axis=0, keepdims=True)
            e = jnp.exp2(s - m)
            expo[t, rows, flat] = e
            gprob[t, rows, flat] = gp
            top[stat : stat + 1, flat] = m
            total[stat : stat + 1, flat] = jnp.sum(e, axis=0, keepdims=True)
            weighted[stat : stat + 1, flat] = jnp.sum(e * gp, axis=0, keepdims=True)

    def relay(t, kt, slot=None, device=None, to=None, cond=None):
        for c in pieces([kt]):
            arrived(t, c)
            if slot is not None:
                send = fwd(slot, got.at[t - 1], device, to, c).start
                if cond is None:
                    send()
                else:
                    when(cond, send)

    def even_step(*kts):
        @pl.when(is_even & (me >= 2))
        def _():
            for t, kt in kts:
                if t == 1:
                    relay(1, kt, 2, me + 2, 3, has_next)
                elif t == 2 and kt in FIRST:
                    relay(2, kt, 3, me + 1, 3)
                elif t == 2:
                    relay(2, kt)
                else:
                    when(me >= 3, functools.partial(relay, 3, kt))

    def odd_step(*kts):
        @pl.when(is_odd)
        def _():
            for t, kt in kts:
                if t == 1 and kt in SECOND:
                    relay(1, kt, 2, me + 2, 3, has_next)
                elif t == 1:
                    relay(1, kt)
                elif t == 2:
                    when(me >= 2, functools.partial(relay, 2, kt, 3, me - 1, 1))
                elif kt in SECOND:
                    when(me >= 2, functools.partial(relay, 3, kt, 4, me - 1, 2))
                else:
                    when(me >= 2, functools.partial(relay, 3, kt))

    def take(t, kt):
        when(me >= t, functools.partial(absorb, t, kt))

    for kt in range(KEY_TILES):
        absorb(0, kt)
    even_step((2, 0))
    odd_step((1, 3), (2, 0))
    take(2, 0)
    even_step((2, 1))
    odd_step((2, 1))
    take(2, 1)
    even_step((1, 0), (2, 2))
    odd_step((2, 2), (1, 0))
    take(1, 0)
    odd_step((2, 3))
    take(2, 2)
    even_step((1, 1))
    odd_step((1, 1))
    take(1, 1)
    even_step((1, 2))
    odd_step((1, 2))
    take(1, 2)
    even_step((1, 3), (3, 0))
    odd_step((3, 3), (3, 0))
    take(1, 3)
    take(3, 0)
    even_step((3, 1))
    odd_step((3, 1))
    take(3, 1)
    even_step((2, 3))
    take(2, 3)
    even_step((3, 2))
    odd_step((3, 2))
    take(3, 2)
    even_step((3, 3))
    take(3, 3)

    best = jnp.max(top[...], axis=0, keepdims=True)
    grow = jnp.exp2(top[...] - best)
    inverse = 1.0 / jnp.sum(grow * total[...], axis=0, keepdims=True)
    factor[...] = grow * inverse
    delta[...] = jnp.sum(grow * weighted[...], axis=0, keepdims=True) * inverse

    def gradients(t, kt):
        r0 = kt * kt_rows
        rows = slice(r0, r0 + kt_rows)
        slot = kt % 2
        stat = t * KEY_TILES + kt
        first = (r0 // qt) * qt if t == 0 else 0
        for h, j, qrows, cols, flat in tiles():
            if j * qt < first:
                continue
            p = expo[t, rows, flat] * factor[stat : stat + 1, flat]
            low_p[slot, :, flat] = p.astype(jnp.bfloat16)
            low_g[slot, :, flat] = (p * (gprob[t, rows, flat] - delta[:, flat])).astype(jnp.bfloat16)
        dk = dv = None
        k_t = block(t)[rows, :hd].T
        for h in range(heads):
            flat = slice(h * tok + first, (h + 1) * tok)
            cols = slice(h * hd, (h + 1) * hd)
            gs = low_g[slot, :, flat]
            dk_h = dot(gs, q_ref[first:, cols])
            dv_h = dot(low_p[slot, :, flat], g_ref[first:, cols])
            dk = dk_h if dk is None else dk + dk_h
            dv = dv_h if dv is None else dv + dv_h
            dq_t[:, flat] += dot(k_t, gs)
        if t == 0:
            own[rows, :hd] = dk
            own[rows, hd:] = dv
        else:
            share[t - 1, rows, :hd] = dk.astype(jnp.bfloat16)
            share[t - 1, rows, hd:] = dv.astype(jnp.bfloat16)

    def bwd(t, device, slot, c):
        return pltpu.make_async_remote_copy(
            src_ref=share.at[t - 1, rows_of(c)], dst_ref=back.at[slot, rows_of(c)],
            send_sem=b_send.at[t - 1, c], recv_sem=b_recv.at[slot, c],
            device_id={"ctx": device}, device_id_type=MESH,
        )

    def returned(slot, c):
        bwd(1, pair, slot, c).wait_recv()

    def merge(t, c):
        returned(t - 1, c)
        rows = rows_of(c)
        both = share[t - 1, rows, :].astype(jnp.float32) + back[t - 1, rows, :].astype(jnp.float32)
        share[t - 1, rows, :] = both.astype(jnp.bfloat16)

    def give(t, kt):
        when(me >= t, functools.partial(gradients, t, kt))

    def send_back(t, kt, device, slot, merged=None):
        for c in pieces([kt]):
            if merged is True:
                merge(t, c)
            elif merged is not None:
                when(merged, functools.partial(merge, t, c))
            bwd(t, device, slot, c).start()

    def even_back(*kts):
        @pl.when(is_even & (me >= 2))
        def _():
            for t, kt in kts:
                if t == 1:
                    send_back(1, kt, me + 1, 1, has_next)
                elif t == 2 and kt in FIRST:
                    send_back(2, kt, me - 2, 4, True)
                elif t == 2:
                    send_back(2, kt, me + 1, 2)
                else:
                    when(me >= 3, functools.partial(send_back, 3, kt, me - 2, 0))

    def odd_back(*kts):
        @pl.when(is_odd)
        def _():
            for t, kt in kts:
                if t == 1:
                    send_back(1, kt, me - 1, 3, has_next if kt in SECOND else None)
                elif t == 2:
                    when(me >= 2, functools.partial(send_back, 2, kt, me - 2, 4, True))
                elif kt in FIRST:
                    when(me >= 2, functools.partial(send_back, 3, kt, me - 1, 1))
                else:
                    when(me >= 2, functools.partial(send_back, 3, kt, me - 2, 0, True))

    give(3, 0)
    even_back((3, 0))
    odd_back((3, 0))
    give(2, 3)
    even_back((2, 3))
    give(3, 1)
    even_back((3, 1))
    odd_back((3, 1))
    give(3, 2)
    even_back((3, 2))
    odd_back((3, 2))
    give(3, 3)
    even_back((3, 3))
    give(1, 0)
    odd_back((1, 0))
    give(1, 1)
    odd_back((1, 1), (3, 3))
    even_back((1, 0))
    give(1, 2)
    odd_back((1, 2))
    give(2, 0)
    even_back((2, 0), (1, 1))
    give(2, 1)
    even_back((2, 1))
    give(2, 2)
    even_back((2, 2))
    give(1, 3)
    gradients(0, 0)
    even_back((1, 2))
    odd_back((2, 0))
    gradients(0, 1)
    odd_back((1, 3))
    gradients(0, 2)
    even_back((1, 3))
    odd_back((2, 1))
    gradients(0, 3)
    odd_back((2, 2))

    for h in range(heads):
        dq_ref[:, h * hd : (h + 1) * hd] = dq_t[:, h * tok : (h + 1) * tok].T.astype(jnp.bfloat16)

    odd_back((2, 3))

    def add_back(slot, c):
        returned(slot, c)
        rows = rows_of(c)
        own[rows, :] += back[slot, rows, :].astype(jnp.float32)

    @pl.when(is_even)
    def _():
        for c in pieces(ALL):
            add_back(3, c)

        @pl.when(has_next)
        def _():
            for c in pieces(FIRST):
                add_back(4, c)

    @pl.when(is_odd & has_next)
    def _():
        for c in pieces(ALL):
            add_back(4, c)

    dkv_ref[...] = own[...].astype(jnp.bfloat16)

    def sent(slot, chunks):
        for c in pieces(chunks):
            fwd(slot, kv_ref, pair, 1, c).wait_send()

    def sent_back(t, chunks):
        for c in pieces(chunks):
            bwd(t, pair, 0, c).wait_send()

    @pl.when(is_even)
    def _():
        sent(0, ALL)

        @pl.when(has_next)
        def _():
            sent(1, FIRST)

        @pl.when(me >= 2)
        def _():
            sent(3, FIRST)

            @pl.when(has_next)
            def _():
                sent(2, ALL)

    @pl.when(is_odd)
    def _():
        @pl.when(has_next)
        def _():
            sent(1, ALL)
            sent(2, SECOND)

        @pl.when(me >= 2)
        def _():
            sent(3, ALL)
            sent(4, SECOND)

    for t in range(1, HOPS + 1):
        when(me >= t, functools.partial(sent_back, t, ALL))


def shards(n, query, key_value, d_out, doc_starts):
    tok, width = query.shape
    hd = key_value.shape[1] // 2
    flat = tok * (width // hd)
    blocks = HOPS + 1
    stats = blocks * KEY_TILES
    bf16, f32 = jnp.bfloat16, jnp.float32
    vmem = pl.BlockSpec(memory_space=pltpu.VMEM)
    pieces = KEY_TILES * SUB
    return pl.pallas_call(
        functools.partial(kernel, n),
        out_shape=(
            jax.ShapeDtypeStruct(query.shape, bf16),
            jax.ShapeDtypeStruct(key_value.shape, bf16),
        ),
        in_specs=[vmem, vmem, vmem, pl.BlockSpec(memory_space=pltpu.SMEM)],
        out_specs=(vmem, vmem),
        scratch_shapes=[
            pltpu.VMEM((HOPS, tok, 2 * hd), bf16),
            pltpu.VMEM((blocks, tok, flat), f32),
            pltpu.VMEM((blocks, tok, flat), f32),
            pltpu.VMEM((stats, flat), f32),
            pltpu.VMEM((stats, flat), f32),
            pltpu.VMEM((stats, flat), f32),
            pltpu.VMEM((stats, flat), f32),
            pltpu.VMEM((1, flat), f32),
            pltpu.VMEM((2, tok // KEY_TILES, flat), bf16),
            pltpu.VMEM((2, tok // KEY_TILES, flat), bf16),
            pltpu.VMEM((hd, flat), f32),
            pltpu.VMEM((tok, 2 * hd), f32),
            pltpu.VMEM((HOPS, tok, 2 * hd), bf16),
            pltpu.VMEM((5, tok, 2 * hd), bf16),
            pltpu.VMEM((1, tok), jnp.int32),
            pltpu.SemaphoreType.DMA((5, pieces)),
            pltpu.SemaphoreType.DMA((HOPS, pieces)),
            pltpu.SemaphoreType.DMA((HOPS, pieces)),
            pltpu.SemaphoreType.DMA((5, pieces)),
        ],
        compiler_params=pltpu.CompilerParams(
            collective_id=0, has_side_effects=True, vmem_limit_bytes=56 * 2**20
        ),
    )(query, d_out, key_value, doc_starts)


def solution(mesh):
    placed = (P("ctx", "head"), P("ctx", "head"), P("ctx", "head"), P("head"))
    return jax.shard_map(
        functools.partial(shards, mesh.shape["ctx"]),
        mesh=mesh,
        in_specs=placed,
        out_specs=(P("ctx", "head"), P("ctx", "head")),
        check_vma=False,
    )
```

```python
import functools
import math

import jax
import jax.numpy as jnp
from jax import lax
from jax.experimental import pallas as pl
from jax.experimental.pallas import tpu as pltpu
from jax.sharding import PartitionSpec as P

HOPS = 3
NEG = -1e30
KEY_TILES = 4
SUB = 2
FIRST, SECOND = range(3), range(3, 4)
MESH = pl.DeviceIdType.MESH


def dot_nt(a, b):
    return lax.dot_general(a, b, (((1,), (1,)), ((), ())), preferred_element_type=jnp.float32)


def dot(a, b):
    return jnp.dot(a, b, preferred_element_type=jnp.float32)


def kernel(
    n, q_in, g_in, kv_in, ds_ref, dq_out, dkv_ref,
    q_ref, g_ref, kv_ref, dq_ref, io_sem,
    got, expo, gprob, top, total, weighted, factor, delta, low_p, low_g, dq_t, own, share, back,
    own_rows, f_send, f_recv, b_send, b_recv,
):
    me = lax.axis_index("ctx")
    odd = lax.rem(me, 2)
    is_odd, is_even = odd == 1, odd == 0
    tok, width = q_ref.shape
    hd = kv_ref.shape[1] // 2
    heads = width // hd
    kt_rows = tok // KEY_TILES
    piece = kt_rows // SUB
    qt = math.gcd(tok, 256)
    scale = hd ** -0.5
    to_log2 = scale * math.log2(math.e)
    has_next = me + 2 < n

    load_kv = pltpu.make_async_copy(kv_in, kv_ref, io_sem.at[0])
    load_q = pltpu.make_async_copy(q_in, q_ref, io_sem.at[1])
    load_g = pltpu.make_async_copy(g_in, g_ref, io_sem.at[2])
    store_dq = pltpu.make_async_copy(dq_ref, dq_out, io_sem.at[3])
    for load in (load_kv, load_q, load_g):
        load.start()

    barrier = pltpu.get_barrier_semaphore()
    pair = me + 1 - 2 * odd

    def greet(device):
        pl.semaphore_signal(barrier, inc=1, device_id={"ctx": device}, device_id_type=MESH)

    greet(pair)

    @pl.when(has_next)
    def _():
        greet(me + 2)

    @pl.when(me >= 2)
    def _():
        greet(me - 2)

    position = me * tok + lax.broadcasted_iota(jnp.int32, (1, tok), 1)
    owners = jnp.zeros((1, tok), jnp.int32)
    for i in range(ds_ref.shape[0]):
        start = ds_ref[i]
        owners = jnp.maximum(owners, jnp.where(position >= start, start, 0))
    own_rows[...] = owners
    top[...] = jnp.full(top.shape, NEG, jnp.float32)
    total[...] = jnp.zeros_like(total)
    weighted[...] = jnp.zeros_like(weighted)
    dq_t[...] = jnp.zeros_like(dq_t)

    @pl.when(has_next & (me >= 2))
    def _():
        pl.semaphore_wait(barrier, 3)

    @pl.when(jnp.logical_not(has_next & (me >= 2)))
    def _():
        pl.semaphore_wait(barrier, 2)

    def rows_of(c):
        return pl.ds(c * piece, piece)

    load_kv.wait()

    def pieces(kts):
        return [kt * SUB + i for kt in kts for i in range(SUB)]

    ALL = range(KEY_TILES)

    def fwd(slot, src, device, t, c):
        return pltpu.make_async_remote_copy(
            src_ref=src.at[rows_of(c)], dst_ref=got.at[t - 1, rows_of(c)],
            send_sem=f_send.at[slot, c], recv_sem=f_recv.at[t - 1, c],
            device_id={"ctx": device}, device_id_type=MESH,
        )

    def arrived(t, c):
        fwd(0, kv_ref, pair, t, c).wait_recv()

    def when(cond, f):
        pl.when(cond)(f)

    @pl.when(is_even)
    def _():
        for c in pieces(SECOND) + pieces(FIRST):
            fwd(0, kv_ref, me + 1, 1, c).start()

        @pl.when(has_next)
        def _():
            for c in pieces(FIRST):
                fwd(1, kv_ref, me + 2, 2, c).start()

    @pl.when(is_odd & has_next)
    def _():
        for c in pieces(ALL):
            fwd(1, kv_ref, me + 2, 2, c).start()

    load_q.wait()
    load_g.wait()

    def tiles():
        for h in range(heads):
            for j in range(tok // qt):
                yield h, j, slice(j * qt, (j + 1) * qt), slice(h * hd, (h + 1) * hd), slice(
                    h * tok + j * qt, h * tok + (j + 1) * qt)

    def block(t):
        return kv_ref if t == 0 else got.at[t - 1]

    def absorb(t, kt):
        r0 = kt * kt_rows
        rows = slice(r0, r0 + kt_rows)
        src = block(t)
        k, v = src[rows, :hd], src[rows, hd:]
        base = (me - t) * tok + r0
        stat = t * KEY_TILES + kt
        key_row = lax.broadcasted_iota(jnp.int32, (kt_rows, qt), 0)
        for h, j, qrows, cols, flat in tiles():
            if t == 0 and (j + 1) * qt <= r0:
                continue
            s = dot_nt(k, q_ref[qrows, cols]) * to_log2
            gp = dot_nt(v, g_ref[qrows, cols]) * scale
            visible = key_row >= own_rows[:, qrows] - base
            if t == 0:
                query_row = lax.broadcasted_iota(jnp.int32, (1, qt), 1) + (j * qt - r0)
                visible = visible & (key_row <= query_row)
            s = jnp.where(visible, s, NEG)
            m = jnp.max(s, axis=0, keepdims=True)
            e = jnp.exp2(s - m)
            expo[t, rows, flat] = e
            gprob[t, rows, flat] = gp
            top[stat : stat + 1, flat] = m
            total[stat : stat + 1, flat] = jnp.sum(e, axis=0, keepdims=True)
            weighted[stat : stat + 1, flat] = jnp.sum(e * gp, axis=0, keepdims=True)

    def relay(t, kt, slot=None, device=None, to=None, cond=None):
        for c in pieces([kt]):
            arrived(t, c)
            if slot is not None:
                send = fwd(slot, got.at[t - 1], device, to, c).start
                if cond is None:
                    send()
                else:
                    when(cond, send)

    def even_step(*kts):
        @pl.when(is_even & (me >= 2))
        def _():
            for t, kt in kts:
                if t == 1:
                    relay(1, kt, 2, me + 2, 3, has_next)
                elif t == 2 and kt in FIRST:
                    relay(2, kt, 3, me + 1, 3)
                elif t == 2:
                    relay(2, kt)
                else:
                    when(me >= 3, functools.partial(relay, 3, kt))

    def odd_step(*kts):
        @pl.when(is_odd)
        def _():
            for t, kt in kts:
                if t == 1 and kt in SECOND:
                    relay(1, kt, 2, me + 2, 3, has_next)
                elif t == 1:
                    relay(1, kt)
                elif t == 2:
                    when(me >= 2, functools.partial(relay, 2, kt, 3, me - 1, 1))
                elif kt in SECOND:
                    when(me >= 2, functools.partial(relay, 3, kt, 4, me - 1, 2))
                else:
                    when(me >= 2, functools.partial(relay, 3, kt))

    def take(t, kt):
        when(me >= t, functools.partial(absorb, t, kt))

    for kt in range(KEY_TILES):
        absorb(0, kt)
    even_step((2, 0))
    odd_step((1, 3), (2, 0))
    take(2, 0)
    even_step((2, 1))
    odd_step((2, 1))
    take(2, 1)
    even_step((1, 0), (2, 2))
    odd_step((2, 2), (1, 0))
    take(1, 0)
    odd_step((2, 3))
    take(2, 2)
    even_step((1, 1))
    odd_step((1, 1))
    take(1, 1)
    even_step((1, 2))
    odd_step((1, 2))
    take(1, 2)
    even_step((1, 3), (3, 0))
    odd_step((3, 3), (3, 0))
    take(1, 3)
    take(3, 0)
    even_step((3, 1))
    odd_step((3, 1))
    take(3, 1)
    even_step((2, 3))
    take(2, 3)
    even_step((3, 2))
    odd_step((3, 2))
    take(3, 2)
    even_step((3, 3))
    take(3, 3)

    best = jnp.max(top[...], axis=0, keepdims=True)
    grow = jnp.exp2(top[...] - best)
    inverse = 1.0 / jnp.sum(grow * total[...], axis=0, keepdims=True)
    factor[...] = grow * inverse
    delta[...] = jnp.sum(grow * weighted[...], axis=0, keepdims=True) * inverse

    def gradients(t, kt):
        r0 = kt * kt_rows
        rows = slice(r0, r0 + kt_rows)
        slot = kt % 2
        stat = t * KEY_TILES + kt
        first = (r0 // qt) * qt if t == 0 else 0
        for h, j, qrows, cols, flat in tiles():
            if j * qt < first:
                continue
            p = expo[t, rows, flat] * factor[stat : stat + 1, flat]
            low_p[slot, :, flat] = p.astype(jnp.bfloat16)
            low_g[slot, :, flat] = (p * (gprob[t, rows, flat] - delta[:, flat])).astype(jnp.bfloat16)
        dk = dv = None
        k_t = block(t)[rows, :hd].T
        for h in range(heads):
            flat = slice(h * tok + first, (h + 1) * tok)
            cols = slice(h * hd, (h + 1) * hd)
            gs = low_g[slot, :, flat]
            dk_h = dot(gs, q_ref[first:, cols])
            dv_h = dot(low_p[slot, :, flat], g_ref[first:, cols])
            dk = dk_h if dk is None else dk + dk_h
            dv = dv_h if dv is None else dv + dv_h
            dq_t[:, flat] += dot(k_t, gs)
        if t == 0:
            own[rows, :hd] = dk
            own[rows, hd:] = dv
        else:
            share[t - 1, rows, :hd] = dk.astype(jnp.bfloat16)
            share[t - 1, rows, hd:] = dv.astype(jnp.bfloat16)

    def bwd(t, device, slot, c):
        return pltpu.make_async_remote_copy(
            src_ref=share.at[t - 1, rows_of(c)], dst_ref=back.at[slot, rows_of(c)],
            send_sem=b_send.at[t - 1, c], recv_sem=b_recv.at[slot, c],
            device_id={"ctx": device}, device_id_type=MESH,
        )

    def returned(slot, c):
        bwd(1, pair, slot, c).wait_recv()

    def merge(t, c):
        returned(t - 1, c)
        rows = rows_of(c)
        both = share[t - 1, rows, :].astype(jnp.float32) + back[t - 1, rows, :].astype(jnp.float32)
        share[t - 1, rows, :] = both.astype(jnp.bfloat16)

    def give(t, kt):
        when(me >= t, functools.partial(gradients, t, kt))

    def send_back(t, kt, device, slot, merged=None):
        for c in pieces([kt]):
            if merged is True:
                merge(t, c)
            elif merged is not None:
                when(merged, functools.partial(merge, t, c))
            bwd(t, device, slot, c).start()

    def even_back(*kts):
        @pl.when(is_even & (me >= 2))
        def _():
            for t, kt in kts:
                if t == 1:
                    send_back(1, kt, me + 1, 1, has_next)
                elif t == 2 and kt in FIRST:
                    send_back(2, kt, me - 2, 4, True)
                elif t == 2:
                    send_back(2, kt, me + 1, 2)
                else:
                    when(me >= 3, functools.partial(send_back, 3, kt, me - 2, 0))

    def odd_back(*kts):
        @pl.when(is_odd)
        def _():
            for t, kt in kts:
                if t == 1:
                    send_back(1, kt, me - 1, 3, has_next if kt in SECOND else None)
                elif t == 2:
                    when(me >= 2, functools.partial(send_back, 2, kt, me - 2, 4, True))
                elif kt in FIRST:
                    when(me >= 2, functools.partial(send_back, 3, kt, me - 1, 1))
                else:
                    when(me >= 2, functools.partial(send_back, 3, kt, me - 2, 0, True))

    give(3, 0)
    even_back((3, 0))
    odd_back((3, 0))
    give(2, 3)
    even_back((2, 3))
    give(3, 1)
    even_back((3, 1))
    odd_back((3, 1))
    give(3, 2)
    even_back((3, 2))
    odd_back((3, 2))
    give(3, 3)
    even_back((3, 3))
    give(1, 0)
    odd_back((1, 0))
    give(1, 1)
    odd_back((1, 1), (3, 3))
    even_back((1, 0))
    give(1, 2)
    odd_back((1, 2))
    give(2, 0)
    even_back((2, 0), (1, 1))
    give(2, 1)
    even_back((2, 1))
    give(2, 2)
    even_back((2, 2))
    give(1, 3)
    gradients(0, 0)
    even_back((1, 2))
    odd_back((2, 0))
    gradients(0, 1)
    odd_back((1, 3))
    gradients(0, 2)
    even_back((1, 3))
    odd_back((2, 1))
    gradients(0, 3)
    odd_back((2, 2))

    for h in range(heads):
        dq_ref[:, h * hd : (h + 1) * hd] = dq_t[:, h * tok : (h + 1) * tok].T.astype(jnp.bfloat16)

    store_dq.start()
    odd_back((2, 3))

    def add_back(slot, c):
        returned(slot, c)
        rows = rows_of(c)
        own[rows, :] += back[slot, rows, :].astype(jnp.float32)

    @pl.when(is_even)
    def _():
        for c in pieces(ALL):
            add_back(3, c)

        @pl.when(has_next)
        def _():
            for c in pieces(FIRST):
                add_back(4, c)

    @pl.when(is_odd & has_next)
    def _():
        for c in pieces(ALL):
            add_back(4, c)

    dkv_ref[...] = own[...].astype(jnp.bfloat16)
    store_dq.wait()

    def sent(slot, chunks):
        for c in pieces(chunks):
            fwd(slot, kv_ref, pair, 1, c).wait_send()

    def sent_back(t, chunks):
        for c in pieces(chunks):
            bwd(t, pair, 0, c).wait_send()

    @pl.when(is_even)
    def _():
        sent(0, ALL)

        @pl.when(has_next)
        def _():
            sent(1, FIRST)

        @pl.when(me >= 2)
        def _():
            sent(3, FIRST)

            @pl.when(has_next)
            def _():
                sent(2, ALL)

    @pl.when(is_odd)
    def _():
        @pl.when(has_next)
        def _():
            sent(1, ALL)
            sent(2, SECOND)

        @pl.when(me >= 2)
        def _():
            sent(3, ALL)
            sent(4, SECOND)

    for t in range(1, HOPS + 1):
        when(me >= t, functools.partial(sent_back, t, ALL))


def shards(n, query, key_value, d_out, doc_starts):
    tok, width = query.shape
    hd = key_value.shape[1] // 2
    flat = tok * (width // hd)
    blocks = HOPS + 1
    stats = blocks * KEY_TILES
    bf16, f32 = jnp.bfloat16, jnp.float32
    vmem = pl.BlockSpec(memory_space=pltpu.VMEM)
    hbm = pl.BlockSpec(memory_space=pl.ANY)
    pieces = KEY_TILES * SUB
    return pl.pallas_call(
        functools.partial(kernel, n),
        out_shape=(
            jax.ShapeDtypeStruct(query.shape, bf16),
            jax.ShapeDtypeStruct(key_value.shape, bf16),
        ),
        in_specs=[hbm, hbm, hbm, pl.BlockSpec(memory_space=pltpu.SMEM)],
        out_specs=(hbm, vmem),
        scratch_shapes=[
            pltpu.VMEM(query.shape, bf16),
            pltpu.VMEM(d_out.shape, bf16),
            pltpu.VMEM(key_value.shape, bf16),
            pltpu.VMEM(query.shape, bf16),
            pltpu.SemaphoreType.DMA((4,)),
            pltpu.VMEM((HOPS, tok, 2 * hd), bf16),
            pltpu.VMEM((blocks, tok, flat), f32),
            pltpu.VMEM((blocks, tok, flat), f32),
            pltpu.VMEM((stats, flat), f32),
            pltpu.VMEM((stats, flat), f32),
            pltpu.VMEM((stats, flat), f32),
            pltpu.VMEM((stats, flat), f32),
            pltpu.VMEM((1, flat), f32),
            pltpu.VMEM((2, tok // KEY_TILES, flat), bf16),
            pltpu.VMEM((2, tok // KEY_TILES, flat), bf16),
            pltpu.VMEM((hd, flat), f32),
            pltpu.VMEM((tok, 2 * hd), f32),
            pltpu.VMEM((HOPS, tok, 2 * hd), bf16),
            pltpu.VMEM((5, tok, 2 * hd), bf16),
            pltpu.VMEM((1, tok), jnp.int32),
            pltpu.SemaphoreType.DMA((5, pieces)),
            pltpu.SemaphoreType.DMA((HOPS, pieces)),
            pltpu.SemaphoreType.DMA((HOPS, pieces)),
            pltpu.SemaphoreType.DMA((5, pieces)),
        ],
        compiler_params=pltpu.CompilerParams(
            collective_id=0, has_side_effects=True, vmem_limit_bytes=56 * 2**20
        ),
    )(query, d_out, key_value, doc_starts)


def solution(mesh):
    placed = (P("ctx", "head"), P("ctx", "head"), P("ctx", "head"), P("head"))
    return jax.shard_map(
        functools.partial(shards, mesh.shape["ctx"]),
        mesh=mesh,
        in_specs=placed,
        out_specs=(P("ctx", "head"), P("ctx", "head")),
        check_vma=False,
    )
```
